256 devices in a mesh: slab: 128 (over x, z, y), sub: 2 (over core).
Axes of the slice: x: 4, y: 4, z: 8, core: 2. Of those that a mesh axis runs over, the one named last changes fastest.
Arguments:
- position: float32 [3, 65536, 128], P(None, ('slab', 'sub')), may hold values from -6 to 6
- state: int32 [65536, 128], P(('slab', 'sub')), may hold values from 0 to 2, as said below
- neighbours: int32 [65536, 8], P(('slab', 'sub')), may hold values from 0 to 65535, as said below
- voxel: int32 [65536, 128], P(('slab', 'sub')), may hold values from 0 to 33554431, as said below
- substrate: float32 [1024, 128, 256], P('slab', 'sub'), may hold values from 0.5 to 1.5
- secretion: float32 [1024, 128, 256], P('slab', 'sub'), may hold values from 0.2 to 4
Outputs:
- new_position: float32 [3, 65536, 128], P(None, ('slab', 'sub'))
- new_substrate: float32 [1024, 128, 256], P('slab', 'sub')
- necrotic_fraction: float32 [], replicated
The draws below stay inside these ranges and needn't reach their ends.
Inputs may be any that keep to these rules, and one draw needn't show every extreme that they name: `state`: 0 marks an empty slot, 1 a live cell, 2 a necrotic cell. `neighbours`: with tiles in blocks of 256 (block t // 256, its slab the block // 2, its part the block % 2): tile t lists itself first, then 8 - 1 different other tiles, each of its own block, of the last 32 tiles of the block 2 blocks before, or of the first 32 tiles of the block 2 blocks after. `voxel`: the cells of a tile of slab s and part u lie in voxels with x from s * 8 to s * 8 + 7 and y from u * 64 to u * 64 + 63.
All inputs are finite; a program needn't handle non-finite values.
Results may differ from the reference program's by a relative error of at most 0.00002.
Values sent between devices are 32-bit elements; how exact they have to be, the bound alone decides.
No kernel may reach another device: no remote copies, remote signals or barrier semaphores. Data moves between devices by JAX's collectives and lax.ppermute only.
A program may use at most 64 MiB of HBM per device.

```python
import math
import jax
import jax.numpy as jnp
from jax import lax

TILE = 128
TILES_DEV = 256
NB = 8
GHOST = 32
VX = 8
VY = 64
VZ = 256
SWEEPS = 8
SLABS = 128
SUB_PARTS = 2
TILES = 65536
NX = 1024
NY = 128
NZ = 256


def draw_state(key, part):
    tile_index = jnp.arange(TILES)
    block_index = tile_index // TILES_DEV
    slab_index = block_index // SUB_PARTS
    blocks = TILES // TILES_DEV
    base_level = jax.random.randint(jax.random.fold_in(key, 2), (), 100, 300)
    block_jitter = jax.random.randint(jax.random.fold_in(key, 3), (blocks,), 700, 1300)
    ramp = 1000 + 2000 * slab_index // max(SLABS - 1, 1)
    threshold = base_level * ramp // 1000 * jnp.take(block_jitter, block_index) // 1000
    necro_base = jax.random.randint(jax.random.fold_in(key, 4), (), 50, 450)
    necro_jitter = jax.random.randint(jax.random.fold_in(key, 5), (blocks,), 600, 1400)
    necro_level = necro_base * jnp.take(necro_jitter, block_index) // 1000
    draw_level = jax.random.randint(key, (TILES, TILE), 0, 1000)
    necrosis = jax.random.randint(jax.random.fold_in(key, 1), (TILES, TILE), 0, 1000)
    return jnp.where(draw_level < threshold[:, None], jnp.where(necrosis < necro_level[:, None], 2, 1), 0).astype(jnp.int32)


def draw_neighbours(key, part):
    width = TILES_DEV + 2 * GHOST
    tile_index = jnp.arange(TILES)[:, None]
    block_index = tile_index // TILES_DEV
    slab_index = block_index // SUB_PARTS
    position_in = tile_index % TILES_DEV
    slot_index = jnp.arange(width)[None, :]
    below = (block_index - SUB_PARTS) * TILES_DEV + TILES_DEV - GHOST + slot_index
    same_block = block_index * TILES_DEV + slot_index - GHOST
    above = (block_index + SUB_PARTS) * TILES_DEV + slot_index - GHOST - TILES_DEV
    candidate = jnp.where(slot_index < GHOST, below, jnp.where(slot_index < GHOST + TILES_DEV, same_block, above))
    usable = jnp.where(slot_index < GHOST, slab_index > 0, jnp.where(slot_index < GHOST + TILES_DEV, slot_index - GHOST != position_in, slab_index < SLABS - 1))
    scores = jax.random.randint(key, (TILES, width), 0, 2 ** 20) * width + slot_index + jnp.where(usable, 0, 2 ** 30)
    ranking = jnp.argsort(scores, axis=1)[:, :NB - 1]
    chosen = jnp.take_along_axis(candidate, ranking, axis=1)
    return jnp.concatenate([tile_index, chosen], 1).astype(jnp.int32)


def draw_voxel(key, part):
    block_index = jnp.arange(TILES)[:, None] // TILES_DEV
    slab_index = block_index // SUB_PARTS
    part_index = block_index % SUB_PARTS
    offset_x = jax.random.randint(jax.random.fold_in(key, 11), (TILES, TILE), 0, VX)
    offset_y = jax.random.randint(jax.random.fold_in(key, 12), (TILES, TILE), 0, VY)
    offset_z = jax.random.randint(jax.random.fold_in(key, 13), (TILES, TILE), 0, VZ)
    return (((slab_index * VX + offset_x) * NY + part_index * VY + offset_y) * NZ + offset_z).astype(jnp.int32)


def block_scale(own_key, shape, pieces, smallest, high):
    def one(dim, shards_of):
        steps = jax.random.uniform(jax.random.fold_in(jax.random.fold_in(own_key, 6), dim), (shards_of,), jnp.float32, smallest / len(pieces), high / len(pieces))
        return jnp.repeat(jnp.exp(steps), shape[dim] // shards_of).reshape((-1,) + (1,) * (len(shape) - dim - 1))

    gain = one(*pieces[0])
    for cut in pieces[1:]:
        gain = gain * one(*cut)
    return gain


def gaussian(stream_key, extent, deviation, limit, split=(), kind=jnp.bfloat16):
    result = deviation * jax.random.normal(stream_key, extent, jnp.float32)
    if split:
        result = result * block_scale(stream_key, extent, split, -0.22, 0.18)
    return jnp.clip(result, -limit, limit).astype(kind)


def setup_inputs(seed: int = 0) -> dict:
    keys = jax.random.split(jax.random.key(seed), 7)
    return {
        "position": gaussian(keys[0], (3, TILES, TILE), 1.0, 6.0, ((1, 256),), jnp.float32),
        "state": draw_state(jax.random.fold_in(keys[6], 71), 0),
        "neighbours": draw_neighbours(jax.random.fold_in(keys[6], 71), 0),
        "voxel": draw_voxel(jax.random.fold_in(keys[6], 71), 0),
        "substrate": jnp.clip(0.5 + 1.0 * jax.random.uniform(keys[4], (NX, NY, NZ), jnp.float32) ** block_scale(keys[4], (NX, NY, NZ), ((0, 128), (1, 2)), -0.2, 0.2), 0.5, 1.5),
        "secretion": jnp.clip(jnp.exp(math.log(4.0) - 2.9957323 * jax.random.uniform(keys[5], (NX, NY, NZ), jnp.float32) ** block_scale(keys[5], (NX, NY, NZ), ((0, 128), (1, 2)), -0.2, 0.2)), 0.2, 4.0),
    }


SOFTENING = 0.01
REPEL_RADIUS = 2.0
ADHERE_RADIUS = 3.0
REPEL_STRENGTH = 0.05
ADHERE_STRENGTH = 0.02
SPEED_LIMIT = 0.2
SPEED_EPSILON = 1e-06
SUBSTRATE_STEP = 0.5
DECAY_RATE = 0.1
DIFFUSION_NUMBER = 2.0
UPTAKE_SCALE = 0.25

def pair_forces(own_tiles, others):
    delta_x = own_tiles[0][:, :, None] - others[0][:, None, :]
    delta_y = own_tiles[1][:, :, None] - others[1][:, None, :]
    delta_z = own_tiles[2][:, :, None] - others[2][:, None, :]
    distance = jnp.sqrt(delta_x * delta_x + delta_y * delta_y + delta_z * delta_z + SOFTENING)
    repel = REPEL_STRENGTH * jnp.square(jnp.maximum(0.0, 1.0 - distance / REPEL_RADIUS))
    adhere = ADHERE_STRENGTH * jnp.square(jnp.maximum(0.0, 1.0 - distance / ADHERE_RADIUS)) * (own_tiles[4][:, :, None] * others[4][:, None, :])
    weight = own_tiles[3][:, :, None] * others[3][:, None, :] * (repel - adhere) / distance
    return jnp.stack([lax.optimization_barrier(jnp.sum(weight * delta_x, -1)), lax.optimization_barrier(jnp.sum(weight * delta_y, -1)), lax.optimization_barrier(jnp.sum(weight * delta_z, -1))], 0)

def neighbour_sum(padded):
    center = padded[1:-1, 1:-1]
    along_z = jnp.pad(center, ((0, 0), (0, 0), (1, 1)))
    return padded[2:, 1:-1] + padded[:-2, 1:-1] + padded[1:-1, 2:] + padded[1:-1, :-2] + along_z[:, :, 2:] + along_z[:, :, :-2]

def reference(position, state, neighbours, voxel, substrate, secretion):
    occupied = (state > 0).astype(jnp.float32)
    living = (state == 1).astype(jnp.float32)
    features = jnp.concatenate([position, occupied[None], living[None]], 0)
    blocks = TILES // TILES_DEV
    own_blocks = features.reshape(5, blocks, TILES_DEV, TILE).transpose(1, 0, 2, 3)
    id_blocks = neighbours.reshape(blocks, TILES_DEV, NB)

    def one_block(block_item):
        own_tiles, tile_ids = block_item
        others = jnp.take(features, tile_ids.reshape(-1), axis=1).reshape(5, TILES_DEV, NB * TILE)
        return pair_forces(own_tiles, others)
    forces = lax.map(one_block, (own_blocks, id_blocks))
    velocity = forces.transpose(1, 0, 2, 3).reshape(3, TILES, TILE)
    cell_speed = jnp.sqrt(lax.optimization_barrier(jnp.sum(velocity * velocity, 0)))
    fastest = jnp.max(cell_speed)
    step_size = SPEED_LIMIT / (fastest + SPEED_EPSILON)
    new_position = position + step_size * velocity
    live_total = jnp.sum((state == 1).astype(jnp.int32)).astype(jnp.int32)
    necrotic_total = jnp.sum((state == 2).astype(jnp.int32)).astype(jnp.int32)
    live_float = live_total.astype(jnp.float32)
    necrotic_float = necrotic_total.astype(jnp.float32)
    per_cell = UPTAKE_SCALE * (NX * NY * NZ) / live_float
    cell_count = jnp.zeros((NX * NY * NZ,), jnp.float32).at[voxel.reshape(-1)].add(living.reshape(-1)).reshape(NX, NY, NZ)
    diagonal = 1.0 + SUBSTRATE_STEP * DECAY_RATE + 6.0 * DIFFUSION_NUMBER + per_cell * cell_count
    right_side = substrate + SUBSTRATE_STEP * secretion
    concentration = substrate
    for sweep_index in range(SWEEPS):
        padded = jnp.pad(concentration, ((1, 1), (1, 1), (0, 0)))
        concentration = (right_side + DIFFUSION_NUMBER * neighbour_sum(padded)) / diagonal
    necrotic_fraction = necrotic_float / (live_float + necrotic_float)
    return (new_position, concentration, necrotic_fraction)
```

```python
import jax
import jax.numpy as jnp
from jax import lax
from jax.experimental import pallas as pl
from jax.experimental.pallas import tpu as pltpu
from jax.sharding import Mesh
from jax.sharding import PartitionSpec as P

TILE = 128
NB = 8
GHOST = 32
SWEEPS = 8
SLAB = ("slab_0", "slab_1", "slab_2")
SLAB_SUB = ("slab_0", "slab_1", "slab_2", "sub")

SOFTENING = 0.01
REPEL_RADIUS = 2.0
ADHERE_RADIUS = 3.0
REPEL_STRENGTH = 0.05
ADHERE_STRENGTH = 0.02
SPEED_LIMIT = 0.2
SPEED_EPSILON = 1e-06
SUBSTRATE_STEP = 0.5
DECAY_RATE = 0.1
DIFFUSION_NUMBER = 2.0
UPTAKE_SCALE = 0.25

FEATURES = 32
FAR = float(2**20)
REPEL_FACTOR = REPEL_STRENGTH / REPEL_RADIUS**2
ADHERE_RATIO = ADHERE_STRENGTH / ADHERE_RADIUS**2 / REPEL_FACTOR
F32 = jnp.float32
BF16 = jnp.bfloat16
VMEM = pltpu.VMEM
VMEM_LIMIT = 60 * 1024 * 1024


def split(x):
    high = x.astype(BF16).astype(F32)
    rest = x - high
    middle = rest.astype(BF16).astype(F32)
    return high, middle, rest - middle


def count_kernel(sub_ref, voxel_ref, state_ref, substrate_ref, secretion_ref, own_ref, edge_ref, count):
    size_x, size_y, size_z = substrate_ref.shape
    grid_y = size_y * 2
    rows = size_x * size_y
    group = 8
    row_id = lax.broadcasted_iota(jnp.int32, (rows, TILE), 0)
    z_id = lax.broadcasted_iota(jnp.int32, (size_z, TILE), 0)
    count[...] = jnp.zeros_like(count)

    def step(g, carry):
        at = pl.multiple_of(g * group, group)
        voxel = voxel_ref[pl.ds(at, group), :]
        live = state_ref[pl.ds(at, group), :] == 1
        z = voxel % size_z
        column = voxel // size_z % size_y
        row = (voxel // (size_z * grid_y) % size_x) * size_y + column
        row = jnp.where(live, row, -1)
        total = None
        for pair in range(0, group, 2):
            left = []
            right = []
            for i in (pair, pair + 1):
                left.append(jnp.where(row_id == row[i : i + 1, :], 1.0, 0.0).astype(BF16))
                right.append(jnp.where(z_id == z[i : i + 1, :], 1.0, 0.0).astype(BF16))
            part = lax.dot_general(
                jnp.concatenate(left, 1),
                jnp.concatenate(right, 1),
                (((1,), (1,)), ((), ())),
                preferred_element_type=F32,
            )
            total = part if total is None else total + part
        count[...] += total
        return carry

    lax.fori_loop(0, voxel_ref.shape[0] // group, step, 0)
    own_ref[0, :, 8 : 8 + size_y, :] = substrate_ref[...]
    own_ref[1, :, 8 : 8 + size_y, :] = secretion_ref[...]
    own_ref[2, :, 8 : 8 + size_y, :] = count[...].reshape(size_x, size_y, size_z)
    edge = pl.multiple_of(8 + (1 - sub_ref[0]) * (size_y - 8), 8)
    edge_ref[...] = own_ref[:, :, pl.ds(edge, 8), :]


def force_kernel(
    ids_ref, own_ref, before_ref, after_ref, velocity_ref, stats_ref,
    features, adhere, weights, left_rows, right_rows, even, odd,
):
    tiles = own_ref.shape[1]
    center = lax.broadcasted_iota(jnp.int32, (FEATURES, TILE), 0)
    ratio = split(jnp.full((FEATURES, TILE), ADHERE_RATIO, F32))
    ratio_rows = jnp.where(
        center == 25, ratio[0], jnp.where(center == 26, ratio[1], jnp.where(center == 27, ratio[2], 0.0))
    ).astype(BF16)
    zero = jnp.zeros((8, TILE), F32)
    one = jnp.ones((8, TILE), F32)

    def put_left(source, at, target):
        state = source[3, pl.ds(at, 8), :]
        live = jnp.where(state == 1.0, 1.0, 0.0)
        vacant = jnp.where(state > 0.5, 0.0, FAR)
        norm = zero
        rows = []
        for axis in range(3):
            value = source[axis, pl.ds(at, 8), :]
            norm = norm + value * value
            high, middle, low = split(value)
            rows += [high, high, high, middle, middle, low]
        rows += [one, one, one]
        rows += list(split(norm))
        rows += [vacant, live, live, live]
        for k, row in enumerate(rows):
            left_rows[k * 8 : k * 8 + 8, :] = row
        for i in range(8):
            block = left_rows[pl.ds(i, FEATURES, stride=8), :]
            turned = block.T.astype(BF16)
            features[target + i] = turned
            adhere[target + i] = jnp.dot(turned, ratio_rows, preferred_element_type=F32)

    def put_right(at):
        norm = jnp.full((8, TILE), SOFTENING, F32)
        for axis in range(3):
            value = own_ref[axis, pl.ds(at, 8), :]
            norm = norm + value * value
            pieces = split(value)
            high, middle, low = [-2.0 * piece for piece in pieces]
            for k, row in enumerate([high, middle, low, high, middle, high]):
                n = axis * 6 + k
                right_rows[0, n * 8 : n * 8 + 8, :] = row
            for k in range(3):
                n = 18 + k
                right_rows[axis + 1, n * 8 : n * 8 + 8, :] = pieces[k]
        for k, row in enumerate(split(norm)):
            n = 18 + k
            right_rows[0, n * 8 : n * 8 + 8, :] = row
        for i in range(8):
            for part in range(4):
                weights[at + i, :, part * TILE : part * TILE + TILE] = right_rows[
                    part, pl.ds(i, FEATURES, stride=8), :
                ].astype(BF16)

    left_rows[...] = jnp.zeros_like(left_rows)
    right_rows[...] = jnp.zeros_like(right_rows)
    for n in range(21, 25):
        right_rows[0, n * 8 : n * 8 + 8, :] = one
    for axis in range(3):
        for k in (0, 3, 5):
            n = axis * 6 + k
            right_rows[axis + 1, n * 8 : n * 8 + 8, :] = -one

    def ghosts(g, carry):
        at = pl.multiple_of(g * 8, 8)
        put_left(before_ref, at, at)
        put_left(after_ref, at, at + GHOST + tiles)
        return carry

    def owned(g, carry):
        at = pl.multiple_of(g * 8, 8)
        put_left(own_ref, at, at + GHOST)
        put_right(at)
        return carry

    lax.fori_loop(0, GHOST // 8, ghosts, 0)
    lax.fori_loop(0, tiles // 8, owned, 0)

    def products(tile, j, target):
        other = ids_ref[tile * NB + j]
        target[j * TILE : (j + 1) * TILE, :] = jnp.dot(
            features[other], weights[tile], preferred_element_type=F32
        )

    def pairs(tile, j, source, reach, total):
        other = ids_ref[tile * NB + j]
        chunk = 32
        for c in range(0, TILE, chunk):
            rows = slice(j * TILE + c, j * TILE + c + chunk)
            square = source[rows, 0:TILE]
            inverse = lax.rsqrt(square)
            distance = square * inverse
            near = jnp.maximum(REPEL_RADIUS - distance, 0.0)
            far = jnp.maximum(reach - distance, 0.0)
            weight = (near * near - adhere[other, c : c + chunk, :] * (far * far)) * inverse
            for axis in range(3):
                term = weight * source[rows, (axis + 1) * TILE : (axis + 2) * TILE]
                total[axis] = total[axis] + jnp.sum(term.reshape(chunk // 8, 8, TILE), 0)
        return total

    def one_tile(tile, following, source, target):
        live = own_ref[3, pl.ds(tile, 1), :] == 1.0
        reach = jnp.broadcast_to(jnp.where(live, ADHERE_RADIUS, -1.0), (32, TILE))
        total = [zero, zero, zero]
        for j in range(NB):
            products(following, j, target)
            total = pairs(tile, j, source, reach, total)
        for axis in range(3):
            velocity_ref[axis, pl.ds(tile, 1), :] = jnp.sum(total[axis], 0, keepdims=True)

    for j in range(NB):
        products(0, j, even)

    def two_tiles(i, carry):
        tile = i * 2
        one_tile(tile, tile + 1, even, odd)
        one_tile(tile + 1, jnp.minimum(tile + 2, tiles - 1), odd, even)
        return carry

    lax.fori_loop(0, tiles // 2, two_tiles, 0)

    state = own_ref[3]
    scale = jnp.where(state > 0.5, REPEL_FACTOR, 0.0)
    speed = jnp.zeros((tiles, TILE), F32)
    for axis in range(3):
        value = velocity_ref[axis] * scale
        velocity_ref[axis] = value
        speed = speed + value * value
    fastest = jnp.max(jnp.sqrt(speed))
    live = jnp.sum(jnp.where(state == 1.0, 1.0, 0.0))
    necrotic = jnp.sum(jnp.where(state == 2.0, 1.0, 0.0))
    lane = lax.broadcasted_iota(jnp.int32, stats_ref.shape, 2)
    stats_ref[...] = jnp.where(lane == 0, fastest, jnp.where(lane == 1, live, necrotic))


def sweep_kernel(
    where_ref, stats_ref, position_ref, velocity_ref, before_ref, own_ref, after_ref,
    new_position_ref, new_substrate_ref, fraction_ref, even, odd, constant, factor,
):
    _, size_x, rows, size_z = own_ref.shape
    size_y = rows - 16
    halves = size_z // TILE
    slab, slabs, subs = where_ref[0], where_ref[1], where_ref[2]
    sub = where_ref[3]
    stats = stats_ref[...]
    lane = lax.broadcasted_iota(jnp.int32, stats.shape, 2)
    fastest = jnp.max(jnp.where(lane == 0, stats, 0.0))
    live = jnp.sum(jnp.where(lane == 1, stats, 0.0))
    necrotic = jnp.sum(jnp.where(lane == 2, stats, 0.0))
    grid_total = size_x * slabs * size_y * subs * size_z
    live_row = jnp.full((8, TILE), live, F32)
    per_cell = UPTAKE_SCALE * jnp.full((8, TILE), grid_total.astype(F32), F32) / live_row
    fraction = jnp.full((8, TILE), necrotic, F32) / (live_row + necrotic)
    fraction_ref[0] = fraction[0, 0]
    step = SPEED_LIMIT / (jnp.full((8, TILE), fastest, F32) + SPEED_EPSILON)
    step_row = step[0:1, :]
    for axis in range(3):
        new_position_ref[axis] = position_ref[axis] + step_row * velocity_ref[axis]
    per_row = per_cell[0:1, :]
    y = lax.broadcasted_iota(jnp.int32, (rows, TILE), 0)
    lowest = jnp.where(sub == 0, 8, 0)
    inside = (y >= lowest) & (y < lowest + size_y + 8)

    def margins(x, carry):
        for field in (even, odd):
            for half in range(halves):
                field[x, half, 0:8, :] = jnp.zeros((8, TILE), F32)
                field[x, half, 8 + rows : 16 + rows, :] = jnp.zeros((8, TILE), F32)
        return carry

    lax.fori_loop(0, 3 * size_x, margins, 0)

    for source, at, present in (
        (before_ref, 0, slab > 0),
        (own_ref, size_x, slab >= 0),
        (after_ref, 2 * size_x, slab < slabs - 1),
    ):
        usable = inside & present

        def fill(x, carry, source=source, at=at, usable=usable):
            base = 1.0 + SUBSTRATE_STEP * DECAY_RATE + 6.0 * DIFFUSION_NUMBER
            for half in range(halves):
                lanes = slice(half * TILE, half * TILE + TILE)
                substrate = source[0, x, :, lanes]
                right_side = substrate + SUBSTRATE_STEP * source[1, x, :, lanes]
                inverse = 1.0 / (base + per_row * source[2, x, :, lanes])
                even[at + x, half, 8 : 8 + rows, :] = jnp.where(usable, substrate, 0.0)
                constant[at + x, half] = jnp.where(usable, right_side * inverse, 0.0)
                factor[at + x, half] = jnp.where(usable, DIFFUSION_NUMBER * inverse, 0.0)
            return carry

        lax.fori_loop(0, size_x, fill, 0)

    low_lane = lax.broadcasted_iota(jnp.int32, (rows, TILE), 1) == 0
    high_lane = lax.broadcasted_iota(jnp.int32, (rows, TILE), 1) == TILE - 1
    here = slice(8, 8 + rows)
    for k in range(SWEEPS):
        source, target = (even, odd) if k % 2 == 0 else (odd, even)
        final = k == SWEEPS - 1

        def sweep(x, carry, source=source, target=target, final=final):
            middle = [source[x, half, here, :] for half in range(halves)]
            right = [pltpu.roll(value, 1, 1) for value in middle]
            left = [pltpu.roll(value, TILE - 1, 1) for value in middle]
            for half in range(halves):
                total = source[x - 1, half, here, :] + source[x + 1, half, here, :]
                total = total + source[x, half, 7 : 7 + rows, :]
                total = total + source[x, half, 9 : 9 + rows, :]
                lower = right[half - 1] if half > 0 else 0.0
                upper = left[half + 1] if half < halves - 1 else 0.0
                total = total + jnp.where(low_lane, lower, right[half])
                total = total + jnp.where(high_lane, upper, left[half])
                value = constant[x, half] + factor[x, half] * total
                if final:
                    new_substrate_ref[x - size_x, :, half * TILE : half * TILE + TILE] = value[8 : 8 + size_y]
                else:
                    target[x, half, here, :] = value
            return carry

        lax.fori_loop(k + 1, 3 * size_x - k - 1, sweep, 0)


WHOLE = pl.BlockSpec(memory_space=pltpu.VMEM)
SCALAR = pl.BlockSpec(memory_space=pltpu.SMEM)


def counts(sub_index, voxel, state, substrate, secretion):
    size_x, size_y, size_z = substrate.shape
    return pl.pallas_call(
        count_kernel,
        out_shape=(
            jax.ShapeDtypeStruct((3, size_x, size_y + 16, size_z), F32),
            jax.ShapeDtypeStruct((3, size_x, 8, size_z), F32),
        ),
        in_specs=[SCALAR] + [WHOLE] * 4,
        out_specs=(WHOLE, WHOLE),
        scratch_shapes=[VMEM((size_x * size_y, size_z), F32)],
        compiler_params=pltpu.CompilerParams(vmem_limit_bytes=VMEM_LIMIT),
        cost_estimate=pl.CostEstimate(flops=9 * 10**9, bytes_accessed=4 * 10**6, transcendentals=0),
        name="counts",
    )(sub_index, voxel, state, substrate, secretion)


def forces(local_ids, codes, ghost_before, ghost_after, devices):
    tiles_dev = codes.shape[1]
    all_tiles = tiles_dev + 2 * GHOST
    return pl.pallas_call(
        force_kernel,
        out_shape=(
            jax.ShapeDtypeStruct((3, tiles_dev, TILE), F32),
            jax.ShapeDtypeStruct((devices, 1, TILE), F32),
        ),
        in_specs=[SCALAR] + [WHOLE] * 3,
        out_specs=(WHOLE, WHOLE),
        scratch_shapes=[
            VMEM((all_tiles, TILE, FEATURES), BF16),
            VMEM((all_tiles, TILE, TILE), F32),
            VMEM((tiles_dev, FEATURES, 4 * TILE), BF16),
            VMEM((FEATURES * 8, TILE), F32),
            VMEM((4, FEATURES * 8, TILE), F32),
            VMEM((NB * TILE, 4 * TILE), F32),
            VMEM((NB * TILE, 4 * TILE), F32),
        ],
        compiler_params=pltpu.CompilerParams(vmem_limit_bytes=VMEM_LIMIT),
        cost_estimate=pl.CostEstimate(flops=10**11, bytes_accessed=10**6, transcendentals=0),
        name="forces",
    )(local_ids, codes, ghost_before, ghost_after)


def sweeps(location, stats, position, velocity, before, own, after):
    _, size_x, rows, size_z = own.shape
    planes = (3 * size_x, size_z // TILE)
    return pl.pallas_call(
        sweep_kernel,
        out_shape=(
            jax.ShapeDtypeStruct(position.shape, F32),
            jax.ShapeDtypeStruct((size_x, rows - 16, size_z), F32),
            jax.ShapeDtypeStruct((1,), F32),
        ),
        in_specs=[SCALAR] + [WHOLE] * 6,
        out_specs=(WHOLE, WHOLE, SCALAR),
        scratch_shapes=[
            VMEM(planes + (rows + 16, TILE), F32),
            VMEM(planes + (rows + 16, TILE), F32),
            VMEM(planes + (rows, TILE), F32),
            VMEM(planes + (rows, TILE), F32),
        ],
        compiler_params=pltpu.CompilerParams(vmem_limit_bytes=VMEM_LIMIT),
        cost_estimate=pl.CostEstimate(flops=10**9, bytes_accessed=8 * 10**6, transcendentals=0),
        name="sweeps",
    )(location, stats, position, velocity, before, own, after)


def body(position, state, neighbours, voxel, substrate, secretion):
    tiles_dev = position.shape[1]
    sub_count = lax.axis_size("sub")
    slab_count = lax.axis_size(SLAB)
    slab_index = lax.axis_index(SLAB)
    sub_index = lax.axis_index("sub")
    device = slab_index * sub_count + sub_index
    size_y = substrate.shape[1]
    up = [(i, i + 1) for i in range(slab_count - 1)]
    down = [(i + 1, i) for i in range(slab_count - 1)]

    codes = jnp.concatenate([position, state.astype(F32)[None]], 0)
    ghost_before = lax.ppermute(codes[:, tiles_dev - GHOST :], SLAB, up)
    ghost_after = lax.ppermute(codes[:, :GHOST], SLAB, down)

    own, edge = counts(sub_index.reshape(1), voxel, state, substrate, secretion)
    other = lax.ppermute(edge, "sub", [(0, 1), (1, 0)])
    own = lax.dynamic_update_slice(own, other, (0, 0, (1 - sub_index) * (size_y + 8), 0))
    field_before = lax.ppermute(own, SLAB, up)
    field_after = lax.ppermute(own, SLAB, down)

    first_tile = device * tiles_dev
    local_ids = jnp.where(
        neighbours < first_tile,
        neighbours - (first_tile - sub_count * tiles_dev) - (tiles_dev - GHOST),
        jnp.where(
            neighbours >= first_tile + tiles_dev,
            GHOST + tiles_dev + neighbours - (first_tile + sub_count * tiles_dev),
            GHOST + neighbours - first_tile,
        ),
    ).reshape(-1)
    velocity, stats = forces(local_ids, codes, ghost_before, ghost_after, slab_count * sub_count)
    stats = lax.all_to_all(stats, SLAB_SUB, 0, 0, tiled=True)
    location = jnp.stack([slab_index, jnp.int32(slab_count), jnp.int32(sub_count), sub_index])
    new_position, new_substrate, fraction = sweeps(
        location, stats, position, velocity, field_before, own, field_after
    )
    return (new_position, new_substrate, fraction.reshape(()))


def solution(mesh):
    finer = Mesh(
        mesh.devices.reshape(4, 8, 4, mesh.shape["sub"]), ("slab_0", "slab_1", "slab_2", "sub")
    )
    placed = (
        P(None, SLAB_SUB, None),
        P(SLAB_SUB, None),
        P(SLAB_SUB, None),
        P(SLAB_SUB, None),
        P(SLAB, "sub", None),
        P(SLAB, "sub", None),
    )
    return jax.shard_map(
        body,
        mesh=finer,
        in_specs=placed,
        out_specs=(P(None, SLAB_SUB, None), P(SLAB, "sub", None), P()),
        check_vma=False,
    )
```

```python
import jax
import jax.numpy as jnp
from jax import lax
from jax.experimental import pallas as pl
from jax.experimental.pallas import tpu as pltpu
from jax.sharding import Mesh
from jax.sharding import PartitionSpec as P

TILE = 128
NB = 8
GHOST = 32
SWEEPS = 8
SLAB = ("slab_0", "slab_1", "slab_2")
SLAB_SUB = ("slab_0", "slab_1", "slab_2", "sub")

SOFTENING = 0.01
REPEL_RADIUS = 2.0
ADHERE_RADIUS = 3.0
REPEL_STRENGTH = 0.05
ADHERE_STRENGTH = 0.02
SPEED_LIMIT = 0.2
SPEED_EPSILON = 1e-06
SUBSTRATE_STEP = 0.5
DECAY_RATE = 0.1
DIFFUSION_NUMBER = 2.0
UPTAKE_SCALE = 0.25

FEATURES = 32
FAR = float(2**20)
REPEL_FACTOR = REPEL_STRENGTH / REPEL_RADIUS**2
ADHERE_RATIO = ADHERE_STRENGTH / ADHERE_RADIUS**2 / REPEL_FACTOR
F32 = jnp.float32
BF16 = jnp.bfloat16
F8 = jnp.float8_e4m3fn
VMEM = pltpu.VMEM
VMEM_LIMIT = 60 * 1024 * 1024


def split(x):
    high = x.astype(BF16).astype(F32)
    rest = x - high
    middle = rest.astype(BF16).astype(F32)
    return high, middle, rest - middle


def count_kernel(sub_ref, voxel_ref, state_ref, substrate_ref, secretion_ref, own_ref, edge_ref, count):
    size_x, size_y, size_z = substrate_ref.shape
    grid_y = size_y * 2
    rows = size_x * size_y
    group = 32
    row_id = lax.broadcasted_iota(jnp.int32, (rows, TILE), 0).astype(jnp.int16)
    z_id = lax.broadcasted_iota(jnp.int32, (size_z, TILE), 0).astype(jnp.int16)
    one_hot, no_hot = jnp.ones((), BF16), jnp.zeros((), BF16)
    count[...] = jnp.zeros_like(count)

    def step(g, carry):
        at = pl.multiple_of(g * group, group)
        voxel = voxel_ref[pl.ds(at, group), :]
        live = state_ref[pl.ds(at, group), :] == 1
        z = voxel % size_z
        column = voxel // size_z % size_y
        row = (voxel // (size_z * grid_y) % size_x) * size_y + column
        row = jnp.where(live, row, -1)
        total = None
        for pair in range(0, group, 2):
            left = []
            right = []
            for i in (pair, pair + 1):
                left.append(jnp.where(row_id == jnp.broadcast_to(row[i : i + 1, :], row_id.shape).astype(jnp.int16), one_hot, no_hot).astype(F8))
                right.append(jnp.where(z_id == jnp.broadcast_to(z[i : i + 1, :], z_id.shape).astype(jnp.int16), one_hot, no_hot).astype(F8))
            part = lax.dot_general(
                jnp.concatenate(left, 1),
                jnp.concatenate(right, 1),
                (((1,), (1,)), ((), ())),
                preferred_element_type=F32,
            )
            total = part if total is None else total + part
        count[...] += total
        return carry

    lax.fori_loop(0, voxel_ref.shape[0] // group, step, 0)
    own_ref[0, :, 8 : 8 + size_y, :] = substrate_ref[...]
    own_ref[1, :, 8 : 8 + size_y, :] = secretion_ref[...]
    own_ref[2, :, 8 : 8 + size_y, :] = count[...].reshape(size_x, size_y, size_z)
    edge = pl.multiple_of(8 + (1 - sub_ref[0]) * (size_y - 8), 8)
    edge_ref[...] = own_ref[:, :, pl.ds(edge, 8), :]


def force_kernel(
    ids_ref, own_ref, before_ref, after_ref, velocity_ref, stats_ref,
    features, adhere, weights, left_rows, right_rows, even, odd,
):
    tiles = own_ref.shape[1]
    center = lax.broadcasted_iota(jnp.int32, (FEATURES, TILE), 0)
    ratio = split(jnp.full((FEATURES, TILE), ADHERE_RATIO, F32))
    ratio_rows = jnp.where(
        center == 25, ratio[0], jnp.where(center == 26, ratio[1], jnp.where(center == 27, ratio[2], 0.0))
    ).astype(BF16)
    zero = jnp.zeros((8, TILE), F32)
    one = jnp.ones((8, TILE), F32)

    def put_left(source, at, target):
        state = source[3, pl.ds(at, 8), :]
        live = jnp.where(state == 1.0, 1.0, 0.0)
        vacant = jnp.where(state > 0.5, 0.0, FAR)
        norm = zero
        rows = []
        for axis in range(3):
            value = source[axis, pl.ds(at, 8), :]
            norm = norm + value * value
            high, middle, low = split(value)
            rows += [high, high, high, middle, middle, low]
        rows += [one, one, one]
        rows += list(split(norm))
        rows += [vacant, live, live, live]
        for k, row in enumerate(rows):
            left_rows[k * 8 : k * 8 + 8, :] = row
        for i in range(8):
            block = left_rows[pl.ds(i, FEATURES, stride=8), :]
            turned = block.T.astype(BF16)
            features[target + i] = turned
            adhere[target + i] = jnp.dot(turned, ratio_rows, preferred_element_type=F32)

    def put_right(at):
        norm = jnp.full((8, TILE), SOFTENING, F32)
        for axis in range(3):
            value = own_ref[axis, pl.ds(at, 8), :]
            norm = norm + value * value
            pieces = split(value)
            high, middle, low = [-2.0 * piece for piece in pieces]
            for k, row in enumerate([high, middle, low, high, middle, high]):
                n = axis * 6 + k
                right_rows[0, n * 8 : n * 8 + 8, :] = row
            for k in range(3):
                n = 18 + k
                right_rows[axis + 1, n * 8 : n * 8 + 8, :] = pieces[k]
        for k, row in enumerate(split(norm)):
            n = 18 + k
            right_rows[0, n * 8 : n * 8 + 8, :] = row
        for i in range(8):
            for part in range(4):
                weights[at + i, :, part * TILE : part * TILE + TILE] = right_rows[
                    part, pl.ds(i, FEATURES, stride=8), :
                ].astype(BF16)

    left_rows[...] = jnp.zeros_like(left_rows)
    right_rows[...] = jnp.zeros_like(right_rows)
    for n in range(21, 25):
        right_rows[0, n * 8 : n * 8 + 8, :] = one
    for axis in range(3):
        for k in (0, 3, 5):
            n = axis * 6 + k
            right_rows[axis + 1, n * 8 : n * 8 + 8, :] = -one

    def ghosts(g, carry):
        at = pl.multiple_of(g * 8, 8)
        put_left(before_ref, at, at)
        put_left(after_ref, at, at + GHOST + tiles)
        return carry

    def owned(g, carry):
        at = pl.multiple_of(g * 8, 8)
        put_left(own_ref, at, at + GHOST)
        put_right(at)
        return carry

    lax.fori_loop(0, GHOST // 8, ghosts, 0)
    lax.fori_loop(0, tiles // 8, owned, 0)

    def products(tile, j, target):
        other = ids_ref[tile * NB + j]
        target[j * TILE : (j + 1) * TILE, :] = jnp.dot(
            features[other], weights[tile], preferred_element_type=F32
        )

    def pairs(tile, j, source, reach, total):
        other = ids_ref[tile * NB + j]
        chunk = 32
        for c in range(0, TILE, chunk):
            rows = slice(j * TILE + c, j * TILE + c + chunk)
            square = source[rows, 0:TILE]
            inverse = lax.rsqrt(square)
            distance = square * inverse
            near = jnp.maximum(REPEL_RADIUS - distance, 0.0)
            far = jnp.maximum(reach - distance, 0.0)
            weight = (near * near - adhere[other, c : c + chunk, :] * (far * far)) * inverse
            for axis in range(3):
                term = weight * source[rows, (axis + 1) * TILE : (axis + 2) * TILE]
                total[axis] = total[axis] + jnp.sum(term.reshape(chunk // 8, 8, TILE), 0)
        return total

    def one_tile(tile, following, source, target):
        live = own_ref[3, pl.ds(tile, 1), :] == 1.0
        reach = jnp.broadcast_to(jnp.where(live, ADHERE_RADIUS, -1.0), (32, TILE))
        total = [zero, zero, zero]
        for j in range(NB):
            products(following, j, target)
            total = pairs(tile, j, source, reach, total)
        for axis in range(3):
            velocity_ref[axis, pl.ds(tile, 1), :] = jnp.sum(total[axis], 0, keepdims=True)

    for j in range(NB):
        products(0, j, even)

    def two_tiles(i, carry):
        tile = i * 2
        one_tile(tile, tile + 1, even, odd)
        one_tile(tile + 1, jnp.minimum(tile + 2, tiles - 1), odd, even)
        return carry

    lax.fori_loop(0, tiles // 2, two_tiles, 0)

    state = own_ref[3]
    scale = jnp.where(state > 0.5, REPEL_FACTOR, 0.0)
    speed = jnp.zeros((tiles, TILE), F32)
    for axis in range(3):
        value = velocity_ref[axis] * scale
        velocity_ref[axis] = value
        speed = speed + value * value
    fastest = jnp.max(jnp.sqrt(speed))
    live = jnp.sum(jnp.where(state == 1.0, 1.0, 0.0))
    necrotic = jnp.sum(jnp.where(state == 2.0, 1.0, 0.0))
    lane = lax.broadcasted_iota(jnp.int32, stats_ref.shape, 2)
    stats_ref[...] = jnp.where(lane == 0, fastest, jnp.where(lane == 1, live, necrotic))


def sweep_kernel(
    where_ref, stats_ref, position_ref, velocity_ref, before_ref, own_ref, after_ref,
    new_position_ref, new_substrate_ref, fraction_ref, even, odd, constant, factor,
):
    _, size_x, rows, size_z = own_ref.shape
    size_y = rows - 16
    halves = size_z // TILE
    slab, slabs, subs = where_ref[0], where_ref[1], where_ref[2]
    sub = where_ref[3]
    stats = stats_ref[...]
    lane = lax.broadcasted_iota(jnp.int32, stats.shape, 2)
    fastest = jnp.max(jnp.where(lane == 0, stats, 0.0))
    live = jnp.sum(jnp.where(lane == 1, stats, 0.0))
    necrotic = jnp.sum(jnp.where(lane == 2, stats, 0.0))
    grid_total = size_x * slabs * size_y * subs * size_z
    live_row = jnp.full((8, TILE), live, F32)
    per_cell = UPTAKE_SCALE * jnp.full((8, TILE), grid_total.astype(F32), F32) / live_row
    fraction = jnp.full((8, TILE), necrotic, F32) / (live_row + necrotic)
    fraction_ref[0] = fraction[0, 0]
    step = SPEED_LIMIT / (jnp.full((8, TILE), fastest, F32) + SPEED_EPSILON)
    step_row = step[0:1, :]
    for axis in range(3):
        new_position_ref[axis] = position_ref[axis] + step_row * velocity_ref[axis]
    per_row = per_cell[0:1, :]
    y = lax.broadcasted_iota(jnp.int32, (rows, TILE), 0)
    lowest = jnp.where(sub == 0, 8, 0)
    inside = (y >= lowest) & (y < lowest + size_y + 8)

    def margins(x, carry):
        for field in (even, odd):
            for half in range(halves):
                field[x, half, 0:8, :] = jnp.zeros((8, TILE), F32)
                field[x, half, 8 + rows : 16 + rows, :] = jnp.zeros((8, TILE), F32)
        return carry

    lax.fori_loop(0, 3 * size_x, margins, 0, unroll=4)

    for source, at, present in (
        (before_ref, 0, slab > 0),
        (own_ref, size_x, slab >= 0),
        (after_ref, 2 * size_x, slab < slabs - 1),
    ):
        usable = inside & present

        def fill(x, carry, source=source, at=at, usable=usable):
            base = 1.0 + SUBSTRATE_STEP * DECAY_RATE + 6.0 * DIFFUSION_NUMBER
            for half in range(halves):
                lanes = slice(half * TILE, half * TILE + TILE)
                substrate = source[0, x, :, lanes]
                right_side = substrate + SUBSTRATE_STEP * source[1, x, :, lanes]
                inverse = 1.0 / (base + per_row * source[2, x, :, lanes])
                even[at + x, half, 8 : 8 + rows, :] = jnp.where(usable, substrate, 0.0)
                constant[at + x, half] = jnp.where(usable, right_side * inverse, 0.0)
                factor[at + x, half] = jnp.where(usable, DIFFUSION_NUMBER * inverse, 0.0)
            return carry

        lax.fori_loop(0, size_x, fill, 0, unroll=4)

    low_lane = lax.broadcasted_iota(jnp.int32, (rows, TILE), 1) == 0
    high_lane = lax.broadcasted_iota(jnp.int32, (rows, TILE), 1) == TILE - 1
    here = slice(8, 8 + rows)
    for k in range(SWEEPS):
        source, target = (even, odd) if k % 2 == 0 else (odd, even)
        final = k == SWEEPS - 1

        def sweep(x, carry, source=source, target=target, final=final):
            middle = [source[x, half, here, :] for half in range(halves)]
            right = [pltpu.roll(value, 1, 1) for value in middle]
            left = [pltpu.roll(value, TILE - 1, 1) for value in middle]
            for half in range(halves):
                total = source[x - 1, half, here, :] + source[x + 1, half, here, :]
                total = total + source[x, half, 7 : 7 + rows, :]
                total = total + source[x, half, 9 : 9 + rows, :]
                lower = right[half - 1] if half > 0 else 0.0
                upper = left[half + 1] if half < halves - 1 else 0.0
                total = total + jnp.where(low_lane, lower, right[half])
                total = total + jnp.where(high_lane, upper, left[half])
                value = constant[x, half] + factor[x, half] * total
                if final:
                    new_substrate_ref[x - size_x, :, half * TILE : half * TILE + TILE] = value[8 : 8 + size_y]
                else:
                    target[x, half, here, :] = value
            return carry

        planes = 3 * size_x - 2 * k - 2
        lax.fori_loop(k + 1, 3 * size_x - k - 1, sweep, 0, unroll=planes // 2)


WHOLE = pl.BlockSpec(memory_space=pltpu.VMEM)
SCALAR = pl.BlockSpec(memory_space=pltpu.SMEM)


def counts(sub_index, voxel, state, substrate, secretion):
    size_x, size_y, size_z = substrate.shape
    return pl.pallas_call(
        count_kernel,
        out_shape=(
            jax.ShapeDtypeStruct((3, size_x, size_y + 16, size_z), F32),
            jax.ShapeDtypeStruct((3, size_x, 8, size_z), F32),
        ),
        in_specs=[SCALAR] + [WHOLE] * 4,
        out_specs=(WHOLE, WHOLE),
        scratch_shapes=[VMEM((size_x * size_y, size_z), F32)],
        compiler_params=pltpu.CompilerParams(vmem_limit_bytes=VMEM_LIMIT),
        cost_estimate=pl.CostEstimate(flops=9 * 10**9, bytes_accessed=4 * 10**6, transcendentals=0),
        name="counts",
    )(sub_index, voxel, state, substrate, secretion)


def forces(local_ids, codes, ghost_before, ghost_after, devices):
    tiles_dev = codes.shape[1]
    all_tiles = tiles_dev + 2 * GHOST
    return pl.pallas_call(
        force_kernel,
        out_shape=(
            jax.ShapeDtypeStruct((3, tiles_dev, TILE), F32),
            jax.ShapeDtypeStruct((devices, 1, TILE), F32),
        ),
        in_specs=[SCALAR] + [WHOLE] * 3,
        out_specs=(WHOLE, WHOLE),
        scratch_shapes=[
            VMEM((all_tiles, TILE, FEATURES), BF16),
            VMEM((all_tiles, TILE, TILE), F32),
            VMEM((tiles_dev, FEATURES, 4 * TILE), BF16),
            VMEM((FEATURES * 8, TILE), F32),
            VMEM((4, FEATURES * 8, TILE), F32),
            VMEM((NB * TILE, 4 * TILE), F32),
            VMEM((NB * TILE, 4 * TILE), F32),
        ],
        compiler_params=pltpu.CompilerParams(vmem_limit_bytes=VMEM_LIMIT),
        cost_estimate=pl.CostEstimate(flops=10**11, bytes_accessed=10**6, transcendentals=0),
        name="forces",
    )(local_ids, codes, ghost_before, ghost_after)


def sweeps(location, stats, position, velocity, before, own, after):
    _, size_x, rows, size_z = own.shape
    planes = (3 * size_x, size_z // TILE)
    return pl.pallas_call(
        sweep_kernel,
        out_shape=(
            jax.ShapeDtypeStruct(position.shape, F32),
            jax.ShapeDtypeStruct((size_x, rows - 16, size_z), F32),
            jax.ShapeDtypeStruct((1,), F32),
        ),
        in_specs=[SCALAR] + [WHOLE] * 6,
        out_specs=(WHOLE, WHOLE, SCALAR),
        scratch_shapes=[
            VMEM(planes + (rows + 16, TILE), F32),
            VMEM(planes + (rows + 16, TILE), F32),
            VMEM(planes + (rows, TILE), F32),
            VMEM(planes + (rows, TILE), F32),
        ],
        compiler_params=pltpu.CompilerParams(vmem_limit_bytes=VMEM_LIMIT),
        cost_estimate=pl.CostEstimate(flops=10**9, bytes_accessed=8 * 10**6, transcendentals=0),
        name="sweeps",
    )(location, stats, position, velocity, before, own, after)


def body(position, state, neighbours, voxel, substrate, secretion):
    tiles_dev = position.shape[1]
    sub_count = lax.axis_size("sub")
    slab_count = lax.axis_size(SLAB)
    slab_index = lax.axis_index(SLAB)
    sub_index = lax.axis_index("sub")
    device = slab_index * sub_count + sub_index
    size_y = substrate.shape[1]
    up = [(i, i + 1) for i in range(slab_count - 1)]
    down = [(i + 1, i) for i in range(slab_count - 1)]

    codes = jnp.concatenate([position, state.astype(F32)[None]], 0)
    ghost_before = lax.ppermute(codes[:, tiles_dev - GHOST :], SLAB, up)
    ghost_after = lax.ppermute(codes[:, :GHOST], SLAB, down)

    own, edge = counts(sub_index.reshape(1), voxel, state, substrate, secretion)
    other = lax.ppermute(edge, "sub", [(0, 1), (1, 0)])
    own = lax.dynamic_update_slice(own, other, (0, 0, (1 - sub_index) * (size_y + 8), 0))
    field_before = lax.ppermute(own, SLAB, up)
    field_after = lax.ppermute(own, SLAB, down)

    first_tile = device * tiles_dev
    local_ids = jnp.where(
        neighbours < first_tile,
        neighbours - (first_tile - sub_count * tiles_dev) - (tiles_dev - GHOST),
        jnp.where(
            neighbours >= first_tile + tiles_dev,
            GHOST + tiles_dev + neighbours - (first_tile + sub_count * tiles_dev),
            GHOST + neighbours - first_tile,
        ),
    ).reshape(-1)
    velocity, stats = forces(local_ids, codes, ghost_before, ghost_after, slab_count * sub_count)
    stats = lax.all_to_all(stats, SLAB_SUB, 0, 0, tiled=True)
    location = jnp.stack([slab_index, jnp.int32(slab_count), jnp.int32(sub_count), sub_index])
    new_position, new_substrate, fraction = sweeps(
        location, stats, position, velocity, field_before, own, field_after
    )
    return (new_position, new_substrate, fraction.reshape(()))


def solution(mesh):
    finer = Mesh(
        mesh.devices.reshape(4, 8, 4, mesh.shape["sub"]), ("slab_0", "slab_1", "slab_2", "sub")
    )
    placed = (
        P(None, SLAB_SUB, None),
        P(SLAB_SUB, None),
        P(SLAB_SUB, None),
        P(SLAB_SUB, None),
        P(SLAB, "sub", None),
        P(SLAB, "sub", None),
    )
    return jax.shard_map(
        body,
        mesh=finer,
        in_specs=placed,
        out_specs=(P(None, SLAB_SUB, None), P(SLAB, "sub", None), P()),
        check_vma=False,
    )
```

```python
import functools

import jax
import jax.numpy as jnp
from jax import lax
from jax.experimental import pallas as pl
from jax.experimental.pallas import tpu as pltpu
from jax.sharding import Mesh
from jax.sharding import PartitionSpec as P

TILE = 128
NB = 8
GHOST = 32
SWEEPS = 8
SLAB = ("slab_0", "slab_1", "slab_2")
SLAB_SUB = ("slab_0", "slab_1", "slab_2", "sub")

SOFTENING = 0.01
REPEL_RADIUS = 2.0
ADHERE_RADIUS = 3.0
REPEL_STRENGTH = 0.05
ADHERE_STRENGTH = 0.02
SPEED_LIMIT = 0.2
SPEED_EPSILON = 1e-06
SUBSTRATE_STEP = 0.5
DECAY_RATE = 0.1
DIFFUSION_NUMBER = 2.0
UPTAKE_SCALE = 0.25

FEATURES = 32
ROW_CHOICES = (48, 64, 80, 96, 112, 128)
FAR = float(2**20)
REPEL_FACTOR = REPEL_STRENGTH / REPEL_RADIUS**2
ADHERE_RATIO = ADHERE_STRENGTH / ADHERE_RADIUS**2 / REPEL_FACTOR
F32 = jnp.float32
BF16 = jnp.bfloat16
F8 = jnp.float8_e4m3fn
VMEM = pltpu.VMEM
VMEM_LIMIT = 60 * 1024 * 1024


def split(x):
    high = x.astype(BF16).astype(F32)
    rest = x - high
    middle = rest.astype(BF16).astype(F32)
    return high, middle, rest - middle


def count_kernel(sub_ref, voxel_ref, state_ref, substrate_ref, secretion_ref, own_ref, edge_ref, count):
    size_x, size_y, size_z = substrate_ref.shape
    grid_y = size_y * 2
    rows = size_x * size_y
    group = 32
    row_id = lax.broadcasted_iota(jnp.int32, (rows, TILE), 0).astype(jnp.int16)
    z_id = lax.broadcasted_iota(jnp.int32, (size_z, TILE), 0).astype(jnp.int16)
    one_hot, no_hot = jnp.ones((), BF16), jnp.zeros((), BF16)
    count[...] = jnp.zeros_like(count)

    def step(g, carry):
        at = pl.multiple_of(g * group, group)
        voxel = voxel_ref[pl.ds(at, group), :]
        live = state_ref[pl.ds(at, group), :] == 1
        z = voxel % size_z
        column = voxel // size_z % size_y
        row = (voxel // (size_z * grid_y) % size_x) * size_y + column
        row = jnp.where(live, row, -1)
        total = None
        for pair in range(0, group, 2):
            left = []
            right = []
            for i in (pair, pair + 1):
                left.append(jnp.where(row_id == jnp.broadcast_to(row[i : i + 1, :], row_id.shape).astype(jnp.int16), one_hot, no_hot).astype(F8))
                right.append(jnp.where(z_id == jnp.broadcast_to(z[i : i + 1, :], z_id.shape).astype(jnp.int16), one_hot, no_hot).astype(F8))
            part = lax.dot_general(
                jnp.concatenate(left, 1),
                jnp.concatenate(right, 1),
                (((1,), (1,)), ((), ())),
                preferred_element_type=F32,
            )
            total = part if total is None else total + part
        count[...] += total
        return carry

    lax.fori_loop(0, voxel_ref.shape[0] // group, step, 0)
    own_ref[0, :, 8 : 8 + size_y, :] = substrate_ref[...]
    own_ref[1, :, 8 : 8 + size_y, :] = secretion_ref[...]
    own_ref[2, :, 8 : 8 + size_y, :] = count[...].reshape(size_x, size_y, size_z)
    edge = pl.multiple_of(8 + (1 - sub_ref[0]) * (size_y - 8), 8)
    edge_ref[...] = own_ref[:, :, pl.ds(edge, 8), :]


def force_kernel(
    ids_ref, own_ref, state_ref, before_ref, after_ref, velocity_ref, stats_ref,
    features, adhere, weights, left_rows, right_rows, even, odd,
):
    tiles = own_ref.shape[1]
    center = lax.broadcasted_iota(jnp.int32, (FEATURES, TILE), 0)
    ratio = split(jnp.full((FEATURES, TILE), ADHERE_RATIO, F32))
    ratio_rows = jnp.where(
        center == 25, ratio[0], jnp.where(center == 26, ratio[1], jnp.where(center == 27, ratio[2], 0.0))
    ).astype(BF16)
    zero = jnp.zeros((8, TILE), F32)
    one = jnp.ones((8, TILE), F32)

    slot = lax.broadcasted_iota(jnp.int32, (8, TILE), 1).astype(F32)
    earlier = jnp.where(
        lax.broadcasted_iota(jnp.int32, (TILE, TILE), 0) < lax.broadcasted_iota(jnp.int32, (TILE, TILE), 1),
        1.0,
        0.0,
    ).astype(BF16)
    place = lax.broadcasted_iota(jnp.int32, (TILE, TILE), 0)

    def put_left(source, state, at, target, fullest):
        occupied = jnp.where(state > 0.5, 1.0, 0.0)
        ahead = jnp.dot(occupied.astype(BF16), earlier, preferred_element_type=F32)
        total = jnp.sum(occupied, 1, keepdims=True)
        order = jnp.where(state > 0.5, ahead, total + slot - ahead).astype(jnp.int32)
        live = jnp.where(state == 1.0, 1.0, 0.0)
        vacant = jnp.where(state > 0.5, 0.0, FAR)
        norm = zero
        rows = []
        for axis in range(3):
            value = source[axis, pl.ds(at, 8), :]
            norm = norm + value * value
            high, middle, low = split(value)
            rows += [high, high, high, middle, middle, low]
        rows += [one, one, one]
        rows += list(split(norm))
        rows += [vacant, live, live, live]
        for k, row in enumerate(rows):
            left_rows[k * 8 : k * 8 + 8, :] = row
        for i in range(8):
            block = left_rows[pl.ds(i, FEATURES, stride=8), :].astype(BF16)
            chosen = jnp.where(place == order[i : i + 1, :], 1.0, 0.0).astype(BF16)
            turned = lax.dot_general(
                chosen, block, (((1,), (1,)), ((), ())), preferred_element_type=F32
            ).astype(BF16)
            features[target + i] = turned
            adhere[target + i] = jnp.dot(turned, ratio_rows, preferred_element_type=F32)
        return jnp.maximum(fullest, ahead + occupied)

    def put_right(at):
        norm = jnp.full((8, TILE), SOFTENING, F32)
        for axis in range(3):
            value = own_ref[axis, pl.ds(at, 8), :]
            norm = norm + value * value
            pieces = split(value)
            high, middle, low = [-2.0 * piece for piece in pieces]
            for k, row in enumerate([high, middle, low, high, middle, high]):
                n = axis * 6 + k
                right_rows[0, n * 8 : n * 8 + 8, :] = row
            for k in range(3):
                n = 18 + k
                right_rows[axis + 1, n * 8 : n * 8 + 8, :] = pieces[k]
        for k, row in enumerate(split(norm)):
            n = 18 + k
            right_rows[0, n * 8 : n * 8 + 8, :] = row
        for i in range(8):
            for part in range(4):
                weights[at + i, :, part * TILE : part * TILE + TILE] = right_rows[
                    part, pl.ds(i, FEATURES, stride=8), :
                ].astype(BF16)

    left_rows[...] = jnp.zeros_like(left_rows)
    right_rows[...] = jnp.zeros_like(right_rows)
    for n in range(21, 25):
        right_rows[0, n * 8 : n * 8 + 8, :] = one
    for axis in range(3):
        for k in (0, 3, 5):
            n = axis * 6 + k
            right_rows[axis + 1, n * 8 : n * 8 + 8, :] = -one

    def ghosts(g, carry):
        at = pl.multiple_of(g * 8, 8)
        carry = put_left(before_ref, before_ref[3, pl.ds(at, 8), :], at, at, carry)
        return put_left(after_ref, after_ref[3, pl.ds(at, 8), :], at, at + GHOST + tiles, carry)

    def owned(g, carry):
        at = pl.multiple_of(g * 8, 8)
        carry = put_left(own_ref, state_ref[pl.ds(at, 8), :].astype(F32), at, at + GHOST, carry)
        put_right(at)
        return carry

    fullest = lax.fori_loop(0, GHOST // 8, ghosts, zero, unroll=2)
    fullest = lax.fori_loop(0, tiles // 8, owned, fullest, unroll=4)
    needed = jnp.max(fullest)

    def run(rows):
        chunk = 16

        def products(tile, j, target):
            other = ids_ref[tile * NB + j]
            target[j * rows : (j + 1) * rows, :] = jnp.dot(
                features[other, 0:rows, :], weights[tile], preferred_element_type=F32
            )

        def pairs(tile, j, source, reach, total):
            other = ids_ref[tile * NB + j]
            for c in range(0, rows, chunk):
                at = slice(j * rows + c, j * rows + c + chunk)
                square = source[at, 0:TILE]
                inverse = lax.rsqrt(square)
                distance = square * inverse
                near = jnp.maximum(REPEL_RADIUS - distance, 0.0)
                far = jnp.maximum(reach - distance, 0.0)
                weight = (near * near - adhere[other, c : c + chunk, :] * (far * far)) * inverse
                for axis in range(3):
                    term = weight * source[at, (axis + 1) * TILE : (axis + 2) * TILE]
                    total[axis] = total[axis] + jnp.sum(term.reshape(chunk // 8, 8, TILE), 0)
            return total

        def one_tile(tile, following, source, target):
            live = state_ref[pl.ds(tile, 1), :] == 1
            reach = jnp.broadcast_to(jnp.where(live, ADHERE_RADIUS, -1.0), (chunk, TILE))
            total = [zero, zero, zero]
            for j in range(NB):
                products(following, j, target)
                total = pairs(tile, j, source, reach, total)
            for axis in range(3):
                velocity_ref[axis, pl.ds(tile, 1), :] = jnp.sum(total[axis], 0, keepdims=True)

        for j in range(NB):
            products(0, j, even)

        def two_tiles(i, carry):
            tile = i * 2
            one_tile(tile, tile + 1, even, odd)
            one_tile(tile + 1, jnp.minimum(tile + 2, tiles - 1), odd, even)
            return carry

        lax.fori_loop(0, tiles // 2, two_tiles, 0)

    below = -1.0
    for rows in ROW_CHOICES:
        pl.when((needed > below) & (needed <= rows))(functools.partial(run, rows))
        below = float(rows)

    state = state_ref[...]
    scale = jnp.where(state > 0, REPEL_FACTOR, 0.0)
    speed = jnp.zeros((tiles, TILE), F32)
    for axis in range(3):
        value = velocity_ref[axis] * scale
        velocity_ref[axis] = value
        speed = speed + value * value
    fastest = jnp.max(jnp.sqrt(speed))
    live = jnp.sum(jnp.where(state == 1, 1.0, 0.0))
    necrotic = jnp.sum(jnp.where(state == 2, 1.0, 0.0))
    lane = lax.broadcasted_iota(jnp.int32, stats_ref.shape, 2)
    stats_ref[...] = jnp.where(lane == 0, fastest, jnp.where(lane == 1, live, necrotic))


def sweep_kernel(
    where_ref, stats_ref, position_ref, velocity_ref, before_ref, own_ref, after_ref,
    new_position_ref, new_substrate_ref, fraction_ref, even, odd, constant, factor,
):
    _, size_x, rows, size_z = own_ref.shape
    size_y = rows - 16
    halves = size_z // TILE
    slab, slabs, subs = where_ref[0], where_ref[1], where_ref[2]
    sub = where_ref[3]
    stats = stats_ref[...]
    lane = lax.broadcasted_iota(jnp.int32, stats.shape, 2)
    fastest = jnp.max(jnp.where(lane == 0, stats, 0.0))
    live = jnp.sum(jnp.where(lane == 1, stats, 0.0))
    necrotic = jnp.sum(jnp.where(lane == 2, stats, 0.0))
    grid_total = size_x * slabs * size_y * subs * size_z
    live_row = jnp.full((8, TILE), live, F32)
    per_cell = UPTAKE_SCALE * jnp.full((8, TILE), grid_total.astype(F32), F32) / live_row
    fraction = jnp.full((8, TILE), necrotic, F32) / (live_row + necrotic)
    fraction_ref[0] = fraction[0, 0]
    step = SPEED_LIMIT / (jnp.full((8, TILE), fastest, F32) + SPEED_EPSILON)
    step_row = step[0:1, :]
    for axis in range(3):
        new_position_ref[axis] = position_ref[axis] + step_row * velocity_ref[axis]
    per_row = per_cell[0:1, :]
    y = lax.broadcasted_iota(jnp.int32, (rows, TILE), 0)
    lowest = jnp.where(sub == 0, 8, 0)
    inside = (y >= lowest) & (y < lowest + size_y + 8)

    def margins(x, carry):
        for field in (even, odd):
            for half in range(halves):
                field[x, half, 0:8, :] = jnp.zeros((8, TILE), F32)
                field[x, half, 8 + rows : 16 + rows, :] = jnp.zeros((8, TILE), F32)
        return carry

    lax.fori_loop(0, 3 * size_x, margins, 0, unroll=4)

    for source, at, present in (
        (before_ref, 0, slab > 0),
        (own_ref, size_x, slab >= 0),
        (after_ref, 2 * size_x, slab < slabs - 1),
    ):
        usable = inside & present

        def fill(x, carry, source=source, at=at, usable=usable):
            base = 1.0 + SUBSTRATE_STEP * DECAY_RATE + 6.0 * DIFFUSION_NUMBER
            for half in range(halves):
                lanes = slice(half * TILE, half * TILE + TILE)
                substrate = source[0, x, :, lanes]
                right_side = substrate + SUBSTRATE_STEP * source[1, x, :, lanes]
                inverse = 1.0 / (base + per_row * source[2, x, :, lanes])
                even[at + x, half, 8 : 8 + rows, :] = jnp.where(usable, substrate, 0.0)
                constant[at + x, half] = jnp.where(usable, right_side * inverse, 0.0)
                factor[at + x, half] = jnp.where(usable, DIFFUSION_NUMBER * inverse, 0.0)
            return carry

        lax.fori_loop(0, size_x, fill, 0, unroll=4)

    low_lane = lax.broadcasted_iota(jnp.int32, (rows, TILE), 1) == 0
    high_lane = lax.broadcasted_iota(jnp.int32, (rows, TILE), 1) == TILE - 1
    here = slice(8, 8 + rows)
    for k in range(SWEEPS):
        source, target = (even, odd) if k % 2 == 0 else (odd, even)
        final = k == SWEEPS - 1

        def sweep(x, carry, source=source, target=target, final=final):
            middle = [source[x, half, here, :] for half in range(halves)]
            right = [pltpu.roll(value, 1, 1) for value in middle]
            left = [pltpu.roll(value, TILE - 1, 1) for value in middle]
            for half in range(halves):
                total = source[x - 1, half, here, :] + source[x + 1, half, here, :]
                total = total + source[x, half, 7 : 7 + rows, :]
                total = total + source[x, half, 9 : 9 + rows, :]
                lower = right[half - 1] if half > 0 else 0.0
                upper = left[half + 1] if half < halves - 1 else 0.0
                total = total + jnp.where(low_lane, lower, right[half])
                total = total + jnp.where(high_lane, upper, left[half])
                value = constant[x, half] + factor[x, half] * total
                if final:
                    new_substrate_ref[x - size_x, :, half * TILE : half * TILE + TILE] = value[8 : 8 + size_y]
                else:
                    target[x, half, here, :] = value
            return carry

        planes = 3 * size_x - 2 * k - 2
        lax.fori_loop(k + 1, 3 * size_x - k - 1, sweep, 0, unroll=planes // 2)


WHOLE = pl.BlockSpec(memory_space=pltpu.VMEM)
SCALAR = pl.BlockSpec(memory_space=pltpu.SMEM)


def counts(sub_index, voxel, state, substrate, secretion):
    size_x, size_y, size_z = substrate.shape
    return pl.pallas_call(
        count_kernel,
        out_shape=(
            jax.ShapeDtypeStruct((3, size_x, size_y + 16, size_z), F32),
            jax.ShapeDtypeStruct((3, size_x, 8, size_z), F32),
        ),
        in_specs=[SCALAR] + [WHOLE] * 4,
        out_specs=(WHOLE, WHOLE),
        scratch_shapes=[VMEM((size_x * size_y, size_z), F32)],
        compiler_params=pltpu.CompilerParams(vmem_limit_bytes=VMEM_LIMIT),
        cost_estimate=pl.CostEstimate(flops=9 * 10**9, bytes_accessed=4 * 10**6, transcendentals=0),
        name="counts",
    )(sub_index, voxel, state, substrate, secretion)


def forces(local_ids, position, state, ghost_before, ghost_after, devices):
    tiles_dev = position.shape[1]
    all_tiles = tiles_dev + 2 * GHOST
    return pl.pallas_call(
        force_kernel,
        out_shape=(
            jax.ShapeDtypeStruct((3, tiles_dev, TILE), F32),
            jax.ShapeDtypeStruct((devices, 1, TILE), F32),
        ),
        in_specs=[SCALAR] + [WHOLE] * 4,
        out_specs=(WHOLE, WHOLE),
        scratch_shapes=[
            VMEM((all_tiles, TILE, FEATURES), BF16),
            VMEM((all_tiles, TILE, TILE), F32),
            VMEM((tiles_dev, FEATURES, 4 * TILE), BF16),
            VMEM((FEATURES * 8, TILE), F32),
            VMEM((4, FEATURES * 8, TILE), F32),
            VMEM((NB * TILE, 4 * TILE), F32),
            VMEM((NB * TILE, 4 * TILE), F32),
        ],
        compiler_params=pltpu.CompilerParams(vmem_limit_bytes=VMEM_LIMIT),
        cost_estimate=pl.CostEstimate(flops=10**11, bytes_accessed=10**6, transcendentals=0),
        name="forces",
    )(local_ids, position, state, ghost_before, ghost_after)


def sweeps(location, stats, position, velocity, before, own, after):
    _, size_x, rows, size_z = own.shape
    planes = (3 * size_x, size_z // TILE)
    return pl.pallas_call(
        sweep_kernel,
        out_shape=(
            jax.ShapeDtypeStruct(position.shape, F32),
            jax.ShapeDtypeStruct((size_x, rows - 16, size_z), F32),
            jax.ShapeDtypeStruct((1,), F32),
        ),
        in_specs=[SCALAR] + [WHOLE] * 6,
        out_specs=(WHOLE, WHOLE, SCALAR),
        scratch_shapes=[
            VMEM(planes + (rows + 16, TILE), F32),
            VMEM(planes + (rows + 16, TILE), F32),
            VMEM(planes + (rows, TILE), F32),
            VMEM(planes + (rows, TILE), F32),
        ],
        compiler_params=pltpu.CompilerParams(vmem_limit_bytes=VMEM_LIMIT),
        cost_estimate=pl.CostEstimate(flops=10**9, bytes_accessed=8 * 10**6, transcendentals=0),
        name="sweeps",
    )(location, stats, position, velocity, before, own, after)


def body(position, state, neighbours, voxel, substrate, secretion):
    tiles_dev = position.shape[1]
    sub_count = lax.axis_size("sub")
    slab_count = lax.axis_size(SLAB)
    slab_index = lax.axis_index(SLAB)
    sub_index = lax.axis_index("sub")
    device = slab_index * sub_count + sub_index
    size_y = substrate.shape[1]
    up = [(i, i + 1) for i in range(slab_count - 1)]
    down = [(i + 1, i) for i in range(slab_count - 1)]

    def codes(tiles):
        return jnp.concatenate([position[:, tiles], state[tiles].astype(F32)[None]], 0)

    ghost_before = lax.ppermute(codes(slice(tiles_dev - GHOST, tiles_dev)), SLAB, up)
    ghost_after = lax.ppermute(codes(slice(0, GHOST)), SLAB, down)

    own, edge = counts(sub_index.reshape(1), voxel, state, substrate, secretion)
    other = lax.ppermute(edge, "sub", [(0, 1), (1, 0)])
    own = lax.dynamic_update_slice(own, other, (0, 0, (1 - sub_index) * (size_y + 8), 0))
    field_before = lax.ppermute(own, SLAB, up)
    field_after = lax.ppermute(own, SLAB, down)

    first_tile = device * tiles_dev
    local_ids = jnp.where(
        neighbours < first_tile,
        neighbours - (first_tile - sub_count * tiles_dev) - (tiles_dev - GHOST),
        jnp.where(
            neighbours >= first_tile + tiles_dev,
            GHOST + tiles_dev + neighbours - (first_tile + sub_count * tiles_dev),
            GHOST + neighbours - first_tile,
        ),
    ).reshape(-1)
    velocity, stats = forces(
        local_ids, position, state, ghost_before, ghost_after, slab_count * sub_count
    )
    stats = lax.all_to_all(stats, SLAB_SUB, 0, 0, tiled=True)
    location = jnp.stack([slab_index, jnp.int32(slab_count), jnp.int32(sub_count), sub_index])
    new_position, new_substrate, fraction = sweeps(
        location, stats, position, velocity, field_before, own, field_after
    )
    return (new_position, new_substrate, fraction.reshape(()))


def solution(mesh):
    finer = Mesh(
        mesh.devices.reshape(4, 8, 4, mesh.shape["sub"]), ("slab_0", "slab_1", "slab_2", "sub")
    )
    placed = (
        P(None, SLAB_SUB, None),
        P(SLAB_SUB, None),
        P(SLAB_SUB, None),
        P(SLAB_SUB, None),
        P(SLAB, "sub", None),
        P(SLAB, "sub", None),
    )
    return jax.shard_map(
        body,
        mesh=finer,
        in_specs=placed,
        out_specs=(P(None, SLAB_SUB, None), P(SLAB, "sub", None), P()),
        check_vma=False,
    )
```

```python
import functools

import jax
import jax.numpy as jnp
from jax import lax
from jax.experimental import pallas as pl
from jax.experimental.pallas import tpu as pltpu
from jax.sharding import Mesh
from jax.sharding import PartitionSpec as P

TILE = 128
NB = 8
GHOST = 32
SWEEPS = 8
SLAB = ("slab_0", "slab_1", "slab_2")
SLAB_SUB = ("slab_0", "slab_1", "slab_2", "sub")

SOFTENING = 0.01
REPEL_RADIUS = 2.0
ADHERE_RADIUS = 3.0
REPEL_STRENGTH = 0.05
ADHERE_STRENGTH = 0.02
SPEED_LIMIT = 0.2
SPEED_EPSILON = 1e-06
SUBSTRATE_STEP = 0.5
DECAY_RATE = 0.1
DIFFUSION_NUMBER = 2.0
UPTAKE_SCALE = 0.25

FEATURES = 32
ROW_CHOICES = (48, 64, 80, 96, 112, 128)
FAR = float(2**20)
REPEL_FACTOR = REPEL_STRENGTH / REPEL_RADIUS**2
ADHERE_RATIO = ADHERE_STRENGTH / ADHERE_RADIUS**2 / REPEL_FACTOR
F32 = jnp.float32
BF16 = jnp.bfloat16
F8 = jnp.float8_e4m3fn
VMEM = pltpu.VMEM
VMEM_LIMIT = 60 * 1024 * 1024


def split(x):
    high = x.astype(BF16).astype(F32)
    rest = x - high
    middle = rest.astype(BF16).astype(F32)
    return high, middle, rest - middle


def count_kernel(sub_ref, voxel_ref, state_ref, substrate_ref, secretion_ref, own_ref, edge_ref, count):
    size_x, size_y, size_z = substrate_ref.shape
    grid_y = size_y * 2
    rows = size_x * size_y
    group = 32
    row_id = lax.broadcasted_iota(jnp.int32, (rows, TILE), 0).astype(jnp.int16)
    z_id = lax.broadcasted_iota(jnp.int32, (size_z, TILE), 0).astype(jnp.int16)
    one_hot, no_hot = jnp.ones((), BF16), jnp.zeros((), BF16)
    count[...] = jnp.zeros_like(count)

    def step(g, carry):
        at = pl.multiple_of(g * group, group)
        voxel = voxel_ref[pl.ds(at, group), :]
        live = state_ref[pl.ds(at, group), :] == 1
        z = voxel % size_z
        column = voxel // size_z % size_y
        row = (voxel // (size_z * grid_y) % size_x) * size_y + column
        row = jnp.where(live, row, -1)
        total = None
        for pair in range(0, group, 2):
            left = []
            right = []
            for i in (pair, pair + 1):
                left.append(jnp.where(row_id == jnp.broadcast_to(row[i : i + 1, :], row_id.shape).astype(jnp.int16), one_hot, no_hot).astype(F8))
                right.append(jnp.where(z_id == jnp.broadcast_to(z[i : i + 1, :], z_id.shape).astype(jnp.int16), one_hot, no_hot).astype(F8))
            part = lax.dot_general(
                jnp.concatenate(left, 1),
                jnp.concatenate(right, 1),
                (((1,), (1,)), ((), ())),
                preferred_element_type=F32,
            )
            total = part if total is None else total + part
        count[...] += total
        return carry

    lax.fori_loop(0, voxel_ref.shape[0] // group, step, 0)
    own_ref[0, :, 8 : 8 + size_y, :] = substrate_ref[...]
    own_ref[1, :, 8 : 8 + size_y, :] = secretion_ref[...]
    own_ref[2, :, 8 : 8 + size_y, :] = count[...].reshape(size_x, size_y, size_z)
    edge = pl.multiple_of(8 + (1 - sub_ref[0]) * (size_y - 8), 8)
    edge_ref[...] = own_ref[:, :, pl.ds(edge, 8), :]


def force_kernel(
    ids_ref, own_ref, state_ref, before_ref, after_ref, velocity_ref, stats_ref,
    features, adhere, weights, left_rows, right_rows, even, odd,
):
    tiles = own_ref.shape[1]
    center = lax.broadcasted_iota(jnp.int32, (FEATURES, TILE), 0)
    ratio = split(jnp.full((FEATURES, TILE), ADHERE_RATIO, F32))
    ratio_rows = jnp.where(
        center == 25, ratio[0], jnp.where(center == 26, ratio[1], jnp.where(center == 27, ratio[2], 0.0))
    ).astype(BF16)
    zero = jnp.zeros((8, TILE), F32)
    one = jnp.ones((8, TILE), F32)

    slot = lax.broadcasted_iota(jnp.int32, (8, TILE), 1).astype(F32)
    earlier = jnp.where(
        lax.broadcasted_iota(jnp.int32, (TILE, TILE), 0) < lax.broadcasted_iota(jnp.int32, (TILE, TILE), 1),
        1.0,
        0.0,
    ).astype(BF16)
    place = lax.broadcasted_iota(jnp.int32, (TILE, TILE), 0)

    def put_left(source, state, at, target, fullest):
        occupied = jnp.where(state > 0.5, 1.0, 0.0)
        ahead = jnp.dot(occupied.astype(BF16), earlier, preferred_element_type=F32)
        total = jnp.sum(occupied, 1, keepdims=True)
        order = jnp.where(state > 0.5, ahead, total + slot - ahead).astype(jnp.int32)
        live = jnp.where(state == 1.0, 1.0, 0.0)
        vacant = jnp.where(state > 0.5, 0.0, FAR)
        norm = zero
        rows = []
        for axis in range(3):
            value = source[axis, pl.ds(at, 8), :]
            norm = norm + value * value
            high, middle, low = split(value)
            rows += [high, high, high, middle, middle, low]
        rows += [one, one, one]
        rows += list(split(norm))
        rows += [vacant, live, live, live]
        for k, row in enumerate(rows):
            left_rows[k * 8 : k * 8 + 8, :] = row
        for i in range(8):
            block = left_rows[pl.ds(i, FEATURES, stride=8), :].astype(BF16)
            chosen = jnp.where(place == order[i : i + 1, :], 1.0, 0.0).astype(BF16)
            turned = lax.dot_general(
                chosen, block, (((1,), (1,)), ((), ())), preferred_element_type=F32
            ).astype(BF16)
            features[target + i] = turned
            adhere[target + i] = jnp.dot(turned, ratio_rows, preferred_element_type=F32)
        return jnp.maximum(fullest, ahead + occupied)

    def put_right(at):
        norm = jnp.full((8, TILE), SOFTENING, F32)
        for axis in range(3):
            value = own_ref[axis, pl.ds(at, 8), :]
            norm = norm + value * value
            pieces = split(value)
            high, middle, low = [-2.0 * piece for piece in pieces]
            for k, row in enumerate([high, middle, low, high, middle, high]):
                n = axis * 6 + k
                right_rows[0, n * 8 : n * 8 + 8, :] = row
            for k in range(3):
                n = 18 + k
                right_rows[axis + 1, n * 8 : n * 8 + 8, :] = pieces[k]
        for k, row in enumerate(split(norm)):
            n = 18 + k
            right_rows[0, n * 8 : n * 8 + 8, :] = row
        for i in range(8):
            for part in range(4):
                weights[at + i, :, part * TILE : part * TILE + TILE] = right_rows[
                    part, pl.ds(i, FEATURES, stride=8), :
                ].astype(BF16)

    left_rows[...] = jnp.zeros_like(left_rows)
    right_rows[...] = jnp.zeros_like(right_rows)
    for n in range(21, 25):
        right_rows[0, n * 8 : n * 8 + 8, :] = one
    for axis in range(3):
        for k in (0, 3, 5):
            n = axis * 6 + k
            right_rows[axis + 1, n * 8 : n * 8 + 8, :] = -one

    def ghosts(g, carry):
        at = pl.multiple_of(g * 8, 8)
        carry = put_left(before_ref, before_ref[3, pl.ds(at, 8), :], at, at, carry)
        return put_left(after_ref, after_ref[3, pl.ds(at, 8), :], at, at + GHOST + tiles, carry)

    def owned(g, carry):
        at = pl.multiple_of(g * 8, 8)
        carry = put_left(own_ref, state_ref[pl.ds(at, 8), :].astype(F32), at, at + GHOST, carry)
        put_right(at)
        return carry

    fullest = lax.fori_loop(0, GHOST // 8, ghosts, zero, unroll=2)
    fullest = lax.fori_loop(0, tiles // 8, owned, fullest, unroll=4)
    needed = jnp.max(fullest)

    def run(rows):
        chunk = 16

        def products(tile, j, target):
            other = ids_ref[tile * NB + j]
            target[j * rows : (j + 1) * rows, :] = jnp.dot(
                features[other, 0:rows, :], weights[tile], preferred_element_type=F32
            )

        def pairs(tile, j, source, reach, total):
            other = ids_ref[tile * NB + j]
            for c in range(0, rows, chunk):
                at = slice(j * rows + c, j * rows + c + chunk)
                square = source[at, 0:TILE]
                inverse = lax.rsqrt(square)
                distance = square * inverse
                near = jnp.maximum(REPEL_RADIUS - distance, 0.0)
                far = jnp.maximum(reach - distance, 0.0)
                weight = (near * near - adhere[other, c : c + chunk, :] * (far * far)) * inverse
                for axis in range(3):
                    term = weight * source[at, (axis + 1) * TILE : (axis + 2) * TILE]
                    total[axis] = total[axis] + jnp.sum(term.reshape(chunk // 8, 8, TILE), 0)
            return total

        def one_tile(tile, following, source, target):
            live = state_ref[pl.ds(tile, 1), :] == 1
            reach = jnp.broadcast_to(jnp.where(live, ADHERE_RADIUS, -1.0), (chunk, TILE))
            total = [zero, zero, zero]
            for j in range(NB):
                products(following, j, target)
                total = pairs(tile, j, source, reach, total)
            for axis in range(3):
                velocity_ref[axis, pl.ds(tile, 1), :] = jnp.sum(total[axis], 0, keepdims=True)

        for j in range(NB):
            products(0, j, even)

        def four_tiles(i, carry):
            tile = i * 4
            one_tile(tile, tile + 1, even, odd)
            one_tile(tile + 1, tile + 2, odd, even)
            one_tile(tile + 2, tile + 3, even, odd)
            one_tile(tile + 3, jnp.minimum(tile + 4, tiles - 1), odd, even)
            return carry

        lax.fori_loop(0, tiles // 4, four_tiles, 0)

    below = -1.0
    for rows in ROW_CHOICES:
        pl.when((needed > below) & (needed <= rows))(functools.partial(run, rows))
        below = float(rows)

    state = state_ref[...]
    scale = jnp.where(state > 0, REPEL_FACTOR, 0.0)
    speed = jnp.zeros((tiles, TILE), F32)
    for axis in range(3):
        value = velocity_ref[axis] * scale
        velocity_ref[axis] = value
        speed = speed + value * value
    fastest = jnp.max(jnp.sqrt(speed))
    live = jnp.sum(jnp.where(state == 1, 1.0, 0.0))
    necrotic = jnp.sum(jnp.where(state == 2, 1.0, 0.0))
    lane = lax.broadcasted_iota(jnp.int32, stats_ref.shape, 2)
    stats_ref[...] = jnp.where(lane == 0, fastest, jnp.where(lane == 1, live, necrotic))


def sweep_kernel(
    where_ref, stats_ref, position_ref, velocity_ref, before_ref, own_ref, after_ref,
    new_position_ref, new_substrate_ref, fraction_ref, even, odd, constant, factor,
):
    _, size_x, rows, size_z = own_ref.shape
    size_y = rows - 16
    halves = size_z // TILE
    slab, slabs, subs = where_ref[0], where_ref[1], where_ref[2]
    sub = where_ref[3]
    stats = stats_ref[...]
    lane = lax.broadcasted_iota(jnp.int32, stats.shape, 2)
    fastest = jnp.max(jnp.where(lane == 0, stats, 0.0))
    live = jnp.sum(jnp.where(lane == 1, stats, 0.0))
    necrotic = jnp.sum(jnp.where(lane == 2, stats, 0.0))
    grid_total = size_x * slabs * size_y * subs * size_z
    live_row = jnp.full((8, TILE), live, F32)
    per_cell = UPTAKE_SCALE * jnp.full((8, TILE), grid_total.astype(F32), F32) / live_row
    fraction = jnp.full((8, TILE), necrotic, F32) / (live_row + necrotic)
    fraction_ref[0] = fraction[0, 0]
    step = SPEED_LIMIT / (jnp.full((8, TILE), fastest, F32) + SPEED_EPSILON)
    step_row = step[0:1, :]
    for axis in range(3):
        new_position_ref[axis] = position_ref[axis] + step_row * velocity_ref[axis]
    per_row = per_cell[0:1, :]
    y = lax.broadcasted_iota(jnp.int32, (rows, TILE), 0)
    lowest = jnp.where(sub == 0, 8, 0)
    inside = (y >= lowest) & (y < lowest + size_y + 8)

    for source, at, present in (
        (before_ref, 0, slab > 0),
        (own_ref, size_x, slab >= 0),
        (after_ref, 2 * size_x, slab < slabs - 1),
    ):
        usable = inside & present

        def fill(x, carry, source=source, at=at, usable=usable):
            base = 1.0 + SUBSTRATE_STEP * DECAY_RATE + 6.0 * DIFFUSION_NUMBER
            for half in range(halves):
                lanes = slice(half * TILE, half * TILE + TILE)
                substrate = source[0, x, :, lanes]
                right_side = substrate + SUBSTRATE_STEP * source[1, x, :, lanes]
                inverse = 1.0 / (base + per_row * source[2, x, :, lanes])
                even[at + x, half] = jnp.where(usable, substrate, 0.0)
                constant[at + x, half] = jnp.where(usable, right_side * inverse, 0.0)
                factor[at + x, half] = jnp.where(usable, DIFFUSION_NUMBER * inverse, 0.0)
            return carry

        lax.fori_loop(0, size_x, fill, 0, unroll=4)

    low_lane = lax.broadcasted_iota(jnp.int32, (rows, TILE), 1) == 0
    high_lane = lax.broadcasted_iota(jnp.int32, (rows, TILE), 1) == TILE - 1
    for k in range(SWEEPS):
        source, target = (even, odd) if k % 2 == 0 else (odd, even)
        final = k == SWEEPS - 1

        def sweep(x, carry, source=source, target=target, final=final):
            middle = [source[x, half] for half in range(halves)]
            right = [pltpu.roll(value, 1, 1) for value in middle]
            left = [pltpu.roll(value, TILE - 1, 1) for value in middle]
            for half in range(halves):
                total = source[x - 1, half] + source[x + 1, half]
                total = total + pltpu.roll(middle[half], 1, 0)
                total = total + pltpu.roll(middle[half], rows - 1, 0)
                lower = right[half - 1] if half > 0 else 0.0
                upper = left[half + 1] if half < halves - 1 else 0.0
                total = total + jnp.where(low_lane, lower, right[half])
                total = total + jnp.where(high_lane, upper, left[half])
                value = constant[x, half] + factor[x, half] * total
                if final:
                    new_substrate_ref[x - size_x, :, half * TILE : half * TILE + TILE] = value[8 : 8 + size_y]
                else:
                    target[x, half] = value
            return carry

        planes = 3 * size_x - 2 * k - 2
        lax.fori_loop(k + 1, 3 * size_x - k - 1, sweep, 0, unroll=planes // 2)


WHOLE = pl.BlockSpec(memory_space=pltpu.VMEM)
SCALAR = pl.BlockSpec(memory_space=pltpu.SMEM)


def counts(sub_index, voxel, state, substrate, secretion):
    size_x, size_y, size_z = substrate.shape
    return pl.pallas_call(
        count_kernel,
        out_shape=(
            jax.ShapeDtypeStruct((3, size_x, size_y + 16, size_z), F32),
            jax.ShapeDtypeStruct((3, size_x, 8, size_z), F32),
        ),
        in_specs=[SCALAR] + [WHOLE] * 4,
        out_specs=(WHOLE, WHOLE),
        scratch_shapes=[VMEM((size_x * size_y, size_z), F32)],
        compiler_params=pltpu.CompilerParams(vmem_limit_bytes=VMEM_LIMIT),
        cost_estimate=pl.CostEstimate(flops=9 * 10**9, bytes_accessed=4 * 10**6, transcendentals=0),
        name="counts",
    )(sub_index, voxel, state, substrate, secretion)


def forces(local_ids, position, state, ghost_before, ghost_after, devices):
    tiles_dev = position.shape[1]
    all_tiles = tiles_dev + 2 * GHOST
    return pl.pallas_call(
        force_kernel,
        out_shape=(
            jax.ShapeDtypeStruct((3, tiles_dev, TILE), F32),
            jax.ShapeDtypeStruct((devices, 1, TILE), F32),
        ),
        in_specs=[SCALAR] + [WHOLE] * 4,
        out_specs=(WHOLE, WHOLE),
        scratch_shapes=[
            VMEM((all_tiles, TILE, FEATURES), BF16),
            VMEM((all_tiles, TILE, TILE), F32),
            VMEM((tiles_dev, FEATURES, 4 * TILE), BF16),
            VMEM((FEATURES * 8, TILE), F32),
            VMEM((4, FEATURES * 8, TILE), F32),
            VMEM((NB * TILE, 4 * TILE), F32),
            VMEM((NB * TILE, 4 * TILE), F32),
        ],
        compiler_params=pltpu.CompilerParams(vmem_limit_bytes=VMEM_LIMIT),
        cost_estimate=pl.CostEstimate(flops=10**11, bytes_accessed=10**6, transcendentals=0),
        name="forces",
    )(local_ids, position, state, ghost_before, ghost_after)


def sweeps(location, stats, position, velocity, before, own, after):
    _, size_x, rows, size_z = own.shape
    planes = (3 * size_x, size_z // TILE)
    return pl.pallas_call(
        sweep_kernel,
        out_shape=(
            jax.ShapeDtypeStruct(position.shape, F32),
            jax.ShapeDtypeStruct((size_x, rows - 16, size_z), F32),
            jax.ShapeDtypeStruct((1,), F32),
        ),
        in_specs=[SCALAR] + [WHOLE] * 6,
        out_specs=(WHOLE, WHOLE, SCALAR),
        scratch_shapes=[
            VMEM(planes + (rows, TILE), F32),
            VMEM(planes + (rows, TILE), F32),
            VMEM(planes + (rows, TILE), F32),
            VMEM(planes + (rows, TILE), F32),
        ],
        compiler_params=pltpu.CompilerParams(vmem_limit_bytes=VMEM_LIMIT),
        cost_estimate=pl.CostEstimate(flops=10**9, bytes_accessed=8 * 10**6, transcendentals=0),
        name="sweeps",
    )(location, stats, position, velocity, before, own, after)


def body(position, state, neighbours, voxel, substrate, secretion):
    tiles_dev = position.shape[1]
    sub_count = lax.axis_size("sub")
    slab_count = lax.axis_size(SLAB)
    slab_index = lax.axis_index(SLAB)
    sub_index = lax.axis_index("sub")
    device = slab_index * sub_count + sub_index
    size_y = substrate.shape[1]
    up = [(i, i + 1) for i in range(slab_count - 1)]
    down = [(i + 1, i) for i in range(slab_count - 1)]

    def codes(tiles):
        return jnp.concatenate([position[:, tiles], state[tiles].astype(F32)[None]], 0)

    ghost_before = lax.ppermute(codes(slice(tiles_dev - GHOST, tiles_dev)), SLAB, up)
    ghost_after = lax.ppermute(codes(slice(0, GHOST)), SLAB, down)

    own, edge = counts(sub_index.reshape(1), voxel, state, substrate, secretion)
    other = lax.ppermute(edge, "sub", [(0, 1), (1, 0)])
    own = lax.dynamic_update_slice(own, other, (0, 0, (1 - sub_index) * (size_y + 8), 0))
    field_before = lax.ppermute(own, SLAB, up)
    field_after = lax.ppermute(own, SLAB, down)

    first_tile = device * tiles_dev
    local_ids = jnp.where(
        neighbours < first_tile,
        neighbours - (first_tile - sub_count * tiles_dev) - (tiles_dev - GHOST),
        jnp.where(
            neighbours >= first_tile + tiles_dev,
            GHOST + tiles_dev + neighbours - (first_tile + sub_count * tiles_dev),
            GHOST + neighbours - first_tile,
        ),
    ).reshape(-1)
    velocity, stats = forces(
        local_ids, position, state, ghost_before, ghost_after, slab_count * sub_count
    )
    stats = lax.all_to_all(stats, SLAB_SUB, 0, 0, tiled=True)
    location = jnp.stack([slab_index, jnp.int32(slab_count), jnp.int32(sub_count), sub_index])
    new_position, new_substrate, fraction = sweeps(
        location, stats, position, velocity, field_before, own, field_after
    )
    return (new_position, new_substrate, fraction.reshape(()))


def solution(mesh):
    finer = Mesh(
        mesh.devices.reshape(4, 8, 4, mesh.shape["sub"]), ("slab_0", "slab_1", "slab_2", "sub")
    )
    placed = (
        P(None, SLAB_SUB, None),
        P(SLAB_SUB, None),
        P(SLAB_SUB, None),
        P(SLAB_SUB, None),
        P(SLAB, "sub", None),
        P(SLAB, "sub", None),
    )
    return jax.shard_map(
        body,
        mesh=finer,
        in_specs=placed,
        out_specs=(P(None, SLAB_SUB, None), P(SLAB, "sub", None), P()),
        check_vma=False,
    )
```
